32 devices in a mesh: expert: 4 (over z), shard: 8 (over y, x, core).
Axes of the slice: x: 2, y: 2, z: 4, core: 2. Of those that a mesh axis runs over, the one named last changes fastest.
Arguments:
- master_gate: float32 [64, 2048, 1408], P('expert', 'shard'), may hold values from -0.1875 to 0.1875
- master_up: float32 [64, 2048, 1408], P('expert', 'shard'), may hold values from -0.1875 to 0.1875
- router_weight: float32 [2048, 64], P('shard', 'expert'), may hold values from -0.125 to 0.125
- router_gain: float32 [2048], P('shard'), may hold values from 0.25 to 1.75
Outputs:
- final_gate: bfloat16 [64, 2048, 1408], P('expert', None, 'shard')
- final_up: bfloat16 [64, 2048, 1408], P('expert', None, 'shard')
- scale_gate: float32 [64, 1408], P('expert', 'shard')
- scale_up: float32 [64, 1408], P('expert', 'shard')
- serve_router: bfloat16 [2048, 64], replicated
The draws below stay inside these ranges and needn't reach their ends.
All inputs are finite; a program needn't handle non-finite values.
Results may differ from the reference program's by a relative error of at most 0.001.
Values may be sent and summed in bfloat16 or wider, within the bound.
No kernel may reach another device: no remote copies, remote signals or barrier semaphores. Data moves between devices by JAX's collectives and lax.ppermute only.
A program may use at most 192 MiB of HBM per device.

```python
import jax
import jax.numpy as jnp
from jax import lax

EXPERTS = 64
D_MODEL = 2048
D_EXPERT = 1408


def strengthened(entries, stream_key, source, target, blocks, factor):
    def block_of(position):
        return (jnp.arange(entries.shape[position]) // (entries.shape[position] // blocks)).reshape((-1,) + (1,) * (entries.ndim - 1 - position))

    one_side = jax.random.permutation(stream_key, blocks)[block_of(target)]
    second = (block_of(target) + blocks // 2) % blocks
    return jnp.where((block_of(source) == one_side) | (block_of(source) == second), factor * entries, entries)


def block_levels(key, dims, pieces, least, top_value):
    def one(position, shards_of):
        heights = jax.random.uniform(jax.random.fold_in(jax.random.fold_in(key, 6), position), (shards_of,), jnp.float32, least / len(pieces), top_value / len(pieces))
        return jnp.repeat(jnp.exp(heights), dims[position] // shards_of).reshape((-1,) + (1,) * (len(dims) - position - 1))

    level = one(*pieces[0])
    for cut in pieces[1:]:
        level = level * one(*cut)
    return level


def bell_draw(own_key, extent, deviation, limit, pieces=(), held_as=jnp.bfloat16):
    result = deviation * jax.random.normal(own_key, extent, jnp.float32)
    if pieces:
        result = result * block_levels(own_key, extent, pieces, -0.22, 0.18)
    return jnp.clip(result, -limit, limit).astype(held_as)


def gaussian_with(rng, shape, width, bound, pieces, heavy, kind=jnp.bfloat16):
    entries = width * jax.random.normal(rng, shape, jnp.float32)
    if pieces:
        entries = entries * block_levels(rng, shape, pieces, -0.22, 0.18)
    return jnp.clip(strengthened(entries, jax.random.fold_in(rng, 3), *heavy), -bound, bound).astype(kind)


def setup_inputs(seed: int = 0) -> dict:
    seeds = jax.random.split(jax.random.key(seed), 5)
    master_gate = gaussian_with(seeds[0], (EXPERTS, D_MODEL, D_EXPERT), D_MODEL ** -0.5, 0.1875, ((0, 4), (1, 8)), (1, 2, 8, 2.0), jnp.float32)
    master_up = gaussian_with(seeds[1], (EXPERTS, D_MODEL, D_EXPERT), D_MODEL ** -0.5, 0.1875, ((0, 4), (1, 8)), (1, 2, 8, 2.0), jnp.float32)
    router_weight = bell_draw(seeds[2], (D_MODEL, EXPERTS), D_MODEL ** -0.5, 0.125, ((0, 8), (1, 4)), jnp.float32)
    router_gain = jnp.clip(1.0 + 0.15 * jax.random.normal(seeds[3], (D_MODEL,), jnp.float32), 0.25, 1.75)
    return dict(master_gate=master_gate, master_up=master_up, router_weight=router_weight, router_gain=router_gain)


def reference(master_gate, master_up, router_weight, router_gain):
    scale_gate = jnp.sqrt(lax.optimization_barrier(jnp.sum(master_gate * master_gate, axis=1)))
    final_gate = (master_gate / jnp.expand_dims(scale_gate, 1)).astype(jnp.bfloat16)
    scale_up = jnp.sqrt(lax.optimization_barrier(jnp.sum(master_up * master_up, axis=1)))
    final_up = (master_up / jnp.expand_dims(scale_up, 1)).astype(jnp.bfloat16)
    serve_router = (router_weight * router_gain[:, None]).astype(jnp.bfloat16)
    return (final_gate, final_up, scale_gate, scale_up, serve_router)
```

```python
import jax
import jax.numpy as jnp
from jax import lax
from jax.experimental import pallas as pl
from jax.experimental.pallas import tpu as pltpu
from jax.sharding import PartitionSpec as P


SPAN = 248.0
HALF = 124.0
TINY = 1e-30
FAR = pl.BlockSpec(memory_space=pltpu.MemorySpace.HBM)


def plain(master_gate, master_up, router_weight, router_gain):
    total_gate, total_up = lax.psum(
        (jnp.sum(master_gate * master_gate, axis=1), jnp.sum(master_up * master_up, axis=1)),
        "shard",
    )
    scale_gate = jnp.sqrt(total_gate)
    scale_up = jnp.sqrt(total_up)
    narrow_gate = (master_gate / jnp.expand_dims(scale_gate, 1)).astype(jnp.bfloat16)
    narrow_up = (master_up / jnp.expand_dims(scale_up, 1)).astype(jnp.bfloat16)
    final_gate = lax.all_to_all(narrow_gate, "shard", split_axis=2, concat_axis=1, tiled=True)
    final_up = lax.all_to_all(narrow_up, "shard", split_axis=2, concat_axis=1, tiled=True)
    mine = lax.axis_index("shard") * final_gate.shape[2]
    scale_gate = lax.dynamic_slice_in_dim(scale_gate, mine, final_gate.shape[2], axis=1)
    scale_up = lax.dynamic_slice_in_dim(scale_up, mine, final_up.shape[2], axis=1)
    part_router = (router_weight * router_gain[:, None]).astype(jnp.bfloat16)
    row_router = lax.all_gather(part_router, "shard", axis=0, tiled=True)
    serve_router = lax.all_gather(row_router, "expert", axis=1, tiled=True)
    return (final_gate, final_up, scale_gate, scale_up, serve_router)


def column_max(x):
    return jnp.max(jnp.abs(x), axis=0, keepdims=True).astype(jnp.bfloat16).astype(jnp.float32)


def encode_kernel(n, piece, *refs):
    x_ref = refs[0]
    outs, turned = refs[-1 - n : -1], refs[-1]
    me = lax.axis_index("shard")
    x = x_ref[0]
    top = column_max(x)
    step = jnp.where(top > TINY, SPAN / jnp.maximum(top, TINY), 0.0)
    y = jnp.exp2(jnp.abs(x) * step - HALF)
    y = jnp.where(x < 0, -y, y)
    turned[...] = y.astype(jnp.bfloat16).T
    for o in range(n):
        first = pl.multiple_of((me ^ o) * piece, 16)
        outs[o][0] = turned[pl.ds(first, piece), :]


def encode(x, first, count, n, after=()):
    _, rows, cols = x.shape
    piece = cols // n
    block = jax.ShapeDtypeStruct((count, piece, rows), jnp.bfloat16)
    return pl.pallas_call(
        lambda *refs: encode_kernel(n, piece, *refs),
        name="encode",
        grid=(count,),
        out_shape=[block] * n,
        in_specs=[pl.BlockSpec((1, rows, cols), lambda i: (first + i, 0, 0))]
        + [FAR] * len(after),
        out_specs=[pl.BlockSpec((1, piece, rows), lambda i: (i, 0, 0))] * n,
        scratch_shapes=[pltpu.VMEM((cols, rows), jnp.bfloat16)],
        cost_estimate=pl.CostEstimate(
            flops=count * 4_000_000, bytes_accessed=count * rows * cols * 6, transcendentals=0
        ),
    )(x, *after)


def stats_kernel(n, piece, experts, *refs):
    gate_ref, up_ref, router_ref, gain_ref = refs[:4]
    outs = refs[-3 - n : -3]
    sums, tops, turned = refs[-3:]
    e = pl.program_id(0)
    me = lax.axis_index("shard")
    for k, ref in enumerate((gate_ref, up_ref)):
        x = ref[0]
        sums[pl.ds(k * experts + e, 1), :] = jnp.sum(x * x, axis=0, keepdims=True)
        tops[pl.ds(k * experts + e, 1), :] = column_max(x)

    @pl.when(e == experts - 1)
    def _():
        total = sums[...]
        high = total.astype(jnp.bfloat16).astype(jnp.float32)
        rest = total - high
        middle = rest.astype(jnp.bfloat16).astype(jnp.float32)
        low = rest - middle
        everything = jnp.concatenate([high, middle, low, tops[...]], axis=0)
        turned[...] = everything.T.astype(jnp.bfloat16)
        router = (router_ref[...] * gain_ref[...]).astype(jnp.bfloat16)
        half = router.shape[1] // 2
        for o in range(n):
            first = pl.multiple_of((me ^ o) * piece, 16)
            outs[o][pl.ds(0, piece), :] = turned[pl.ds(first, piece), :]
            outs[o][pl.ds(piece, experts), :] = router[:, :half]
            outs[o][pl.ds(piece + experts, experts), :] = router[:, half:]


def stats(gate, up, router, gain, n, after=()):
    experts, rows, cols = gate.shape
    piece = cols // n
    block = jax.ShapeDtypeStruct((piece + 2 * experts, 128), jnp.bfloat16)
    whole = pl.BlockSpec(memory_space=pltpu.VMEM)
    return pl.pallas_call(
        lambda *refs: stats_kernel(n, piece, experts, *refs),
        name="stats",
        grid=(experts,),
        out_shape=[block] * n,
        in_specs=[pl.BlockSpec((1, rows, cols), lambda i: (i, 0, 0))] * 2
        + [whole] * 2
        + [FAR] * len(after),
        out_specs=[whole] * n,
        scratch_shapes=[
            pltpu.VMEM((2 * experts, cols), jnp.float32),
            pltpu.VMEM((2 * experts, cols), jnp.float32),
            pltpu.VMEM((cols, 128), jnp.bfloat16),
        ],
        cost_estimate=pl.CostEstimate(
            flops=experts * 4_000_000, bytes_accessed=experts * rows * cols * 8, transcendentals=0
        ),
    )(gate, up, router, gain, *after)


def factor_kernel(n, piece, experts, rows, *refs):
    told = refs[:n]
    factor_ref, gate_ref, up_ref, router_ref = refs[n:]
    me = lax.axis_index("shard")
    w = 2 * experts
    half = rows // 2
    total, tops = None, []
    for o in range(n):
        lines = told[o][pl.ds(0, piece), :].astype(jnp.float32).T
        part = lines[:w] + lines[w : 2 * w] + lines[2 * w : 3 * w]
        total = part if total is None else total + part
        tops.append(lines[3 * w : 4 * w])
        for k in range(2):
            at = pl.multiple_of((me ^ o) * rows + k * half, half)
            router_ref[:, pl.ds(at, half)] = told[o][pl.ds(piece + k * experts, experts), :]
    scale = jnp.sqrt(total)
    gate_ref[...] = scale[:experts]
    up_ref[...] = scale[experts:]
    for o in range(n):
        factor_ref[:, o, :] = tops[o] / (SPAN * scale)


def factors(told, experts, rows, router_kind):
    n = len(told)
    piece = told[0].shape[0] - 2 * experts
    return pl.pallas_call(
        lambda *refs: factor_kernel(n, piece, experts, rows, *refs),
        name="factors",
        out_shape=[
            jax.ShapeDtypeStruct((2 * experts, n, piece), jnp.float32),
            jax.ShapeDtypeStruct((experts, piece), jnp.float32),
            jax.ShapeDtypeStruct((experts, piece), jnp.float32),
            jax.ShapeDtypeStruct((experts, n * rows), router_kind),
        ],
        cost_estimate=pl.CostEstimate(
            flops=2_000_000, bytes_accessed=3_000_000, transcendentals=0
        ),
    )(*told)


def decode_kernel(n, rows, *refs):
    factor_ref, pieces, out_ref, token_ref = refs[0], refs[1 : 1 + n], refs[-2], refs[-1]
    token_ref[...] = jnp.zeros_like(token_ref)
    me = lax.axis_index("shard")
    factor = factor_ref[0].T
    for o in range(n):
        y = pieces[o][0].astype(jnp.float32)
        v = (jnp.log2(jnp.abs(y)) + HALF) * factor[:, o : o + 1]
        v = jnp.where(y < 0, -v, v).astype(jnp.bfloat16)
        first = pl.multiple_of((me ^ o) * rows, 128)
        out_ref[0, :, pl.ds(first, rows)] = v


def decode(pieces, factor, which, first, experts, into):
    n = len(pieces)
    count, piece, rows = pieces[0].shape
    base = which * experts + first
    into = () if into is None else (into,)
    return pl.pallas_call(
        lambda *refs: decode_kernel(n, rows, *refs),
        name="decode",
        grid=(count,),
        out_shape=[
            jax.ShapeDtypeStruct((experts, piece, n * rows), jnp.bfloat16),
            jax.ShapeDtypeStruct((8, 128), jnp.float32),
        ],
        in_specs=[pl.BlockSpec((1, n, piece), lambda i: (base + i, 0, 0))]
        + [pl.BlockSpec((1, piece, rows), lambda i: (i, 0, 0))] * n
        + [FAR] * len(into),
        out_specs=[
            pl.BlockSpec((1, piece, n * rows), lambda i: (first + i, 0, 0)),
            pl.BlockSpec((8, 128), lambda i: (0, 0)),
        ],
        input_output_aliases={n + 1: 0} if into else {},
        cost_estimate=pl.CostEstimate(
            flops=count * 4_000_000, bytes_accessed=count * rows * piece * n * 4, transcendentals=0
        ),
    )(factor, *pieces, *into)


def place_kernel(axis, along, n, part, *refs):
    me = lax.axis_index(axis)
    out_ref = refs[-1]
    for o in range(n):
        first = pl.multiple_of((me ^ o) * part, part)
        at = (slice(None), pl.ds(first, part)) if along else (pl.ds(first, part), slice(None))
        out_ref[at] = refs[o][...]


def place(parts, axis, along):
    n = len(parts)
    shape = list(parts[0].shape)
    part = shape[along]
    shape[along] *= n
    return pl.pallas_call(
        lambda *refs: place_kernel(axis, along, n, part, *refs),
        name="place",
        out_shape=jax.ShapeDtypeStruct(tuple(shape), parts[0].dtype),
    )(*parts)


def swap(x, axis, n, o):
    return lax.ppermute(x, axis, [(i, i ^ o) for i in range(n)])


ORDER = (2, 4, 6, 3, 5, 7, 1)


def exchange(parts):
    n = len(parts)
    got = [parts[0]] + [None] * (n - 1)
    order = ORDER if n == 8 else range(1, n)
    for o in order:
        got[o] = swap(parts[o], "shard", n, o)
    return got


def cuts(experts):
    sizes, left = [], experts
    step = max(1, experts // 4)
    while left > 0:
        sizes.append(min(step, left))
        left -= sizes[-1]
    return sizes


def plan(experts):
    if experts == 16:
        sizes = ([2, 5, 5, 4], [5, 5, 5, 1])
    else:
        sizes = (cuts(experts), cuts(experts))
    chunks = []
    for which in range(2):
        first = 0
        for size in sizes[which]:
            chunks.append((which, first, size))
            first += size
    return chunks


AHEAD = 2


def local(groups, n, gate, up, router_weight, router_gain):
    experts, rows, _ = gate.shape
    chunks = plan(experts)
    source = (gate, up)
    result = [None, None]
    got, tokens = {}, {}

    def send(k):
        which, first, size = chunks[k]
        after = ()
        if k >= AHEAD:
            after += tuple(got[k - AHEAD][1:])
        if k - AHEAD - 1 in tokens:
            after += (tokens[k - AHEAD - 1],)
        sent = encode(source[which], first, size, n, after)
        got[k] = exchange(sent)

    def receive(k):
        which, first, _ = chunks[k]
        result[which], tokens[k] = decode(
            got[k], factor, which, first, experts, result[which]
        )

    for k in range(AHEAD):
        send(k)
    messages = stats(gate, up, router_weight.T, router_gain[None, :], n)
    messages = exchange(messages)
    factor, scale_gate, scale_up, rows_router = factors(messages, experts, rows, jnp.bfloat16)
    blocks = [rows_router] + [
        swap(rows_router, "expert", groups, o) for o in range(1, groups)
    ]
    serve_router = place(blocks, "expert", 0).T
    for k in range(AHEAD, len(chunks)):
        send(k)
        receive(k - AHEAD)
    for k in range(len(chunks) - AHEAD, len(chunks)):
        receive(k)
    return (
        result[0].transpose(0, 2, 1),
        result[1].transpose(0, 2, 1),
        scale_gate,
        scale_up,
        serve_router,
    )


def power_of_two(n):
    return n & (n - 1) == 0


def suits(groups, n, experts, rows, cols):
    return (
        power_of_two(n)
        and power_of_two(groups)
        and n <= 16
        and cols % (16 * n) == 0
        and cols % 128 == 0
        and rows == 256
        and experts == 16
    )


def solution(mesh):
    groups, n = mesh.shape["expert"], mesh.shape["shard"]

    def body(gate, up, router_weight, router_gain):
        if gate.shape == up.shape and suits(groups, n, *gate.shape):
            return local(groups, n, gate, up, router_weight, router_gain)
        return plain(gate, up, router_weight, router_gain)

    in_specs = (
        P("expert", "shard", None),
        P("expert", "shard", None),
        P("shard", "expert"),
        P("shard"),
    )
    out_specs = (
        P("expert", None, "shard"),
        P("expert", None, "shard"),
        P("expert", "shard"),
        P("expert", "shard"),
        P(),
    )
    step = jax.shard_map(body, mesh=mesh, in_specs=in_specs, out_specs=out_specs, check_vma=False)

    def whole(master_gate, master_up, router_weight, router_gain):
        experts, rows, cols = master_gate.shape
        run = step
        if suits(groups, n, experts // groups, rows // n, cols):
            run = step
        return run(master_gate, master_up, router_weight, router_gain)

    return whole
```

```python
import jax
import jax.numpy as jnp
from jax import lax
from jax.experimental import pallas as pl
from jax.experimental.pallas import tpu as pltpu
from jax.sharding import PartitionSpec as P


SPAN = 248.0
HALF = 124.0
TINY = 1.2e-19
LEAST, RATE, DEEP = 0.05, 240.0 / 8.2, 120.0
FAR = pl.BlockSpec(memory_space=pltpu.MemorySpace.HBM)


def plain(master_gate, master_up, router_weight, router_gain):
    total_gate, total_up = lax.psum(
        (jnp.sum(master_gate * master_gate, axis=1), jnp.sum(master_up * master_up, axis=1)),
        "shard",
    )
    scale_gate = jnp.sqrt(total_gate)
    scale_up = jnp.sqrt(total_up)
    narrow_gate = (master_gate / jnp.expand_dims(scale_gate, 1)).astype(jnp.bfloat16)
    narrow_up = (master_up / jnp.expand_dims(scale_up, 1)).astype(jnp.bfloat16)
    final_gate = lax.all_to_all(narrow_gate, "shard", split_axis=2, concat_axis=1, tiled=True)
    final_up = lax.all_to_all(narrow_up, "shard", split_axis=2, concat_axis=1, tiled=True)
    mine = lax.axis_index("shard") * final_gate.shape[2]
    scale_gate = lax.dynamic_slice_in_dim(scale_gate, mine, final_gate.shape[2], axis=1)
    scale_up = lax.dynamic_slice_in_dim(scale_up, mine, final_up.shape[2], axis=1)
    part_router = (router_weight * router_gain[:, None]).astype(jnp.bfloat16)
    row_router = lax.all_gather(part_router, "shard", axis=0, tiled=True)
    serve_router = lax.all_gather(row_router, "expert", axis=1, tiled=True)
    return (final_gate, final_up, scale_gate, scale_up, serve_router)


def column_max(x):
    return jnp.max(jnp.abs(x), axis=0, keepdims=True).astype(jnp.bfloat16).astype(jnp.float32)


def offsets(n):
    return (0, 2, 4, 6, 3, 5, 7, 1) if n == 8 else tuple(range(n))


def encode_kernel(n, piece, *refs):
    x_ref = refs[0]
    outs, turned = refs[-1 - n : -1], refs[-1]
    me = lax.axis_index("shard")
    x = x_ref[0]
    top = column_max(x)
    step = jnp.where(top > TINY, SPAN / jnp.maximum(top, TINY), 0.0)
    y = jnp.exp2(jnp.abs(x) * step - HALF)
    y = jnp.where(x < 0, -y, y)
    turned[...] = y.astype(jnp.bfloat16).T
    for k, o in enumerate(offsets(n)):
        first = pl.multiple_of((me ^ o) * piece, 16)
        outs[k][0] = turned[pl.ds(first, piece), :]


def encode(x, first, count, n, after=()):
    _, rows, cols = x.shape
    piece = cols // n
    block = jax.ShapeDtypeStruct((count, piece, rows), jnp.bfloat16)
    return pl.pallas_call(
        lambda *refs: encode_kernel(n, piece, *refs),
        name="encode",
        grid=(count,),
        out_shape=[block] * n,
        in_specs=[pl.BlockSpec((1, rows, cols), lambda i: (first + i, 0, 0))]
        + [FAR] * len(after),
        out_specs=[pl.BlockSpec((1, piece, rows), lambda i: (i, 0, 0))] * n,
        scratch_shapes=[pltpu.VMEM((cols, rows), jnp.bfloat16)],
        cost_estimate=pl.CostEstimate(
            flops=count * 4_000_000, bytes_accessed=count * rows * cols * 6, transcendentals=0
        ),
    )(x, *after)


def stats_kernel(n, piece, experts, *refs):
    gate_ref, up_ref, router_ref, gain_ref = refs[:4]
    outs = refs[-3 - n : -3]
    sums, tops, turned = refs[-3:]
    e = pl.program_id(0)
    me = lax.axis_index("shard")
    for k, ref in enumerate((gate_ref, up_ref)):
        x = ref[0]
        sums[pl.ds(k * experts + e, 1), :] = jnp.sum(x * x, axis=0, keepdims=True)
        tops[pl.ds(k * experts + e, 1), :] = column_max(x)

    @pl.when(e == experts - 1)
    def _():
        top = tops[...]
        ratio = jnp.where(top > TINY, sums[...] / jnp.maximum(top * top, TINY * TINY), 1.0)
        code = jnp.exp2((jnp.log2(ratio) + LEAST) * RATE - DEEP)
        both = jnp.concatenate([code, top], axis=0)
        turned[...] = jnp.concatenate([both, both], axis=0).T
        router = (router_ref[...] * gain_ref[...]).astype(jnp.bfloat16)
        half = router.shape[1] // 2
        short = piece // 2
        lane = lax.broadcasted_iota(jnp.int32, (short, 128), 1)
        for k, o in enumerate(offsets(n)):
            first = pl.multiple_of((me ^ o) * piece, 8)
            one = turned[pl.ds(first, short), :]
            two = turned[pl.ds(pl.multiple_of(first + short, 8), short), :]
            outs[k][pl.ds(0, experts), :] = router[:, :half]
            outs[k][pl.ds(experts, experts), :] = router[:, half:]
            packed = jnp.where(lane < 64, one, two).astype(jnp.bfloat16)
            outs[k][pl.ds(2 * experts, short), :] = packed


def stats(gate, up, router, gain, n, after=()):
    experts, rows, cols = gate.shape
    piece = cols // n
    block = jax.ShapeDtypeStruct((piece // 2 + 2 * experts, 128), jnp.bfloat16)
    whole = pl.BlockSpec(memory_space=pltpu.VMEM)
    return pl.pallas_call(
        lambda *refs: stats_kernel(n, piece, experts, *refs),
        name="stats",
        grid=(experts,),
        out_shape=[block] * n,
        in_specs=[pl.BlockSpec((1, rows, cols), lambda i: (i, 0, 0))] * 2
        + [whole] * 2
        + [FAR] * len(after),
        out_specs=[whole] * n,
        scratch_shapes=[
            pltpu.VMEM((2 * experts, cols), jnp.float32),
            pltpu.VMEM((2 * experts, cols), jnp.float32),
            pltpu.VMEM((cols, 128), jnp.float32),
        ],
        cost_estimate=pl.CostEstimate(
            flops=experts * 4_000_000, bytes_accessed=experts * rows * cols * 8, transcendentals=0
        ),
    )(gate, up, router, gain, *after)


def factor_kernel(n, piece, experts, rows, *refs):
    told = refs[:n]
    factor_ref, gate_ref, up_ref, router_ref = refs[n:]
    me = lax.axis_index("shard")
    w = 2 * experts
    half, short = rows // 2, piece // 2
    total, tops = None, []
    for k, o in enumerate(offsets(n)):
        lines = told[k][pl.ds(2 * experts, short), :].astype(jnp.float32).T
        lines = jnp.concatenate([lines[: 2 * w], lines[2 * w :]], axis=1)
        top = lines[w:]
        ratio = jnp.exp2((jnp.log2(lines[:w]) + DEEP) / RATE - LEAST)
        part = ratio * (top * top)
        total = part if total is None else total + part
        tops.append(top)
        for h in range(2):
            at = pl.multiple_of((me ^ o) * rows + h * half, half)
            router_ref[:, pl.ds(at, half)] = told[k][pl.ds(h * experts, experts), :]
    scale = jnp.sqrt(total)
    gate_ref[...] = scale[:experts]
    up_ref[...] = scale[experts:]
    for k in range(n):
        factor_ref[:, k, :] = tops[k] / (SPAN * scale)


def factors(told, experts, rows, router_kind):
    n = len(told)
    piece = 2 * (told[0].shape[0] - 2 * experts)
    return pl.pallas_call(
        lambda *refs: factor_kernel(n, piece, experts, rows, *refs),
        name="factors",
        out_shape=[
            jax.ShapeDtypeStruct((2 * experts, n, piece), jnp.float32),
            jax.ShapeDtypeStruct((experts, piece), jnp.float32),
            jax.ShapeDtypeStruct((experts, piece), jnp.float32),
            jax.ShapeDtypeStruct((experts, n * rows), router_kind),
        ],
        cost_estimate=pl.CostEstimate(
            flops=2_000_000, bytes_accessed=3_000_000, transcendentals=0
        ),
    )(*told)


def decode_kernel(n, rows, *refs):
    factor_ref, pieces, out_ref, token_ref = refs[0], refs[1 : 1 + n], refs[-2], refs[-1]
    token_ref[...] = jnp.zeros_like(token_ref)
    me = lax.axis_index("shard")
    factor = factor_ref[0].T
    for k, o in enumerate(offsets(n)):
        first = pl.multiple_of((me ^ o) * rows, 128)
        out_ref[0, :, pl.ds(first, rows)] = decoded(pieces[k][0], factor[:, k : k + 1])


def decoded(y, factor):
    y = y.astype(jnp.float32)
    v = (jnp.log2(jnp.abs(y)) + HALF) * factor
    return jnp.where(y < 0, -v, v).astype(jnp.bfloat16)


def decode(pieces, factor, which, first, experts, into):
    n = len(pieces)
    count, piece, rows = pieces[0].shape
    base = which * experts + first
    into = () if into is None else (into,)
    return pl.pallas_call(
        lambda *refs: decode_kernel(n, rows, *refs),
        name="decode",
        grid=(count,),
        out_shape=[
            jax.ShapeDtypeStruct((experts, piece, n * rows), jnp.bfloat16),
            jax.ShapeDtypeStruct((8, 128), jnp.float32),
        ],
        in_specs=[pl.BlockSpec((1, n, piece), lambda i: (base + i, 0, 0))]
        + [pl.BlockSpec((1, piece, rows), lambda i: (i, 0, 0))] * n
        + [FAR] * len(into),
        out_specs=[
            pl.BlockSpec((1, piece, n * rows), lambda i: (first + i, 0, 0)),
            pl.BlockSpec((8, 128), lambda i: (0, 0)),
        ],
        input_output_aliases={n + 1: 0} if into else {},
        cost_estimate=pl.CostEstimate(
            flops=count * 4_000_000, bytes_accessed=count * rows * piece * n * 4, transcendentals=0
        ),
    )(factor, *pieces, *into)


def finish_kernel(n, some, base, which, rows, *refs):
    factor_ref, pieces = refs[0], refs[1 : 1 + len(some)]
    out_ref, token_ref, ready, sems = refs[-4:]
    token_ref[...] = jnp.zeros_like(token_ref)
    me = lax.axis_index("shard")
    factor = factor_ref[base].T
    copies = []
    for at, k in enumerate(some):
        first = pl.multiple_of((me ^ offsets(n)[k]) * rows, 128)
        ready[at] = decoded(pieces[at][0], factor[:, k : k + 1])
        copies.append(
            pltpu.make_async_copy(
                ready.at[at], out_ref.at[which, :, pl.ds(first, rows)], sems.at[at]
            )
        )
        copies[-1].start()
    for copy in copies:
        copy.wait()


def finish(pieces, some, factor, base, which, into):
    n = factor.shape[1]
    _, piece, rows = pieces[0].shape
    near = pl.BlockSpec(memory_space=pltpu.MemorySpace.VMEM)
    return pl.pallas_call(
        lambda *refs: finish_kernel(n, some, base, which, rows, *refs),
        name="finish",
        out_shape=[
            jax.ShapeDtypeStruct(into.shape, into.dtype),
            jax.ShapeDtypeStruct((8, 128), jnp.float32),
        ],
        in_specs=[near] * (1 + len(some)) + [FAR],
        out_specs=[FAR, near],
        scratch_shapes=[
            pltpu.VMEM((len(some), piece, rows), jnp.bfloat16),
            pltpu.SemaphoreType.DMA((len(some),)),
        ],
        input_output_aliases={len(some) + 1: 0},
        compiler_params=pltpu.CompilerParams(vmem_limit_bytes=8 * 1024 * 1024),
        cost_estimate=pl.CostEstimate(
            flops=500_000 * len(some),
            bytes_accessed=rows * piece * len(some) * 4,
            transcendentals=0,
        ),
    )(factor, *pieces, into)


def place_kernel(axis, along, n, part, *refs):
    me = lax.axis_index(axis)
    out_ref = refs[-1]
    for o in range(n):
        first = pl.multiple_of((me ^ o) * part, part)
        at = (slice(None), pl.ds(first, part)) if along else (pl.ds(first, part), slice(None))
        out_ref[at] = refs[o][...]


def place(parts, axis, along):
    n = len(parts)
    shape = list(parts[0].shape)
    part = shape[along]
    shape[along] *= n
    return pl.pallas_call(
        lambda *refs: place_kernel(axis, along, n, part, *refs),
        name="place",
        out_shape=jax.ShapeDtypeStruct(tuple(shape), parts[0].dtype),
    )(*parts)


def swap(x, axis, n, o):
    return lax.ppermute(x, axis, [(i, i ^ o) for i in range(n)])


def exchange(parts):
    n = len(parts)
    return [parts[0]] + [
        swap(parts[k], "shard", n, o) for k, o in enumerate(offsets(n)) if o
    ]


def cuts(experts):
    sizes, left = [], experts
    step = max(1, experts // 4)
    while left > 0:
        sizes.append(min(step, left))
        left -= sizes[-1]
    return sizes


def plan(experts):
    if experts == 16:
        sizes = ([2, 5, 5, 4], [5, 5, 3, 2, 1])
    else:
        sizes = (cuts(experts), cuts(experts))
    chunks = []
    for which in range(2):
        first = 0
        for size in sizes[which]:
            chunks.append((which, first, size))
            first += size
    return chunks


AHEAD = 2


def local(groups, n, gate, up, router_weight, router_gain):
    experts, rows, _ = gate.shape
    chunks = plan(experts)
    source = (gate, up)
    result = [None, None]
    got, tokens = {}, {}

    def send(k):
        which, first, size = chunks[k]
        after = ()
        if k >= AHEAD:
            after += tuple(got[k - AHEAD][1:])
        if k - AHEAD - 1 in tokens:
            after += (tokens[k - AHEAD - 1],)
        if k == AHEAD + 3:
            after += (placed,)
        sent = encode(source[which], first, size, n, after)
        got[k] = exchange(sent)

    def receive(k):
        which, first, size = chunks[k]
        if size == 1 and k == len(chunks) - 1:
            base = which * experts + first
            late = tuple(range(n // 2, n - 1))
            soon = tuple(range(n // 2)) + (n - 1,)
            for some in (soon, late):
                pieces = [got[k][j] for j in some]
                result[which], tokens[k] = finish(pieces, some, factor, base, first, result[which])
            return
        result[which], tokens[k] = decode(
            got[k], factor, which, first, experts, result[which]
        )

    for k in range(AHEAD):
        send(k)
    messages = stats(gate, up, router_weight.T, router_gain[None, :], n)
    messages = exchange(messages)
    factor, scale_gate, scale_up, rows_router = factors(messages, experts, rows, jnp.bfloat16)
    blocks = [rows_router] + [
        swap(rows_router, "expert", groups, o) for o in range(1, groups)
    ]
    placed = place(blocks, "expert", 0)
    for k in range(AHEAD, len(chunks)):
        send(k)
        receive(k - AHEAD)
    for k in range(len(chunks) - AHEAD, len(chunks)):
        receive(k)
    return (
        result[0].transpose(0, 2, 1),
        result[1].transpose(0, 2, 1),
        scale_gate,
        scale_up,
        placed.T,
    )


def power_of_two(n):
    return n & (n - 1) == 0


def suits(groups, n, experts, rows, cols):
    return (
        power_of_two(n)
        and power_of_two(groups)
        and n <= 16
        and cols % (16 * n) == 0
        and cols % 128 == 0
        and rows == 256
        and experts == 16
    )


def solution(mesh):
    groups, n = mesh.shape["expert"], mesh.shape["shard"]

    def body(gate, up, router_weight, router_gain):
        if gate.shape == up.shape and suits(groups, n, *gate.shape):
            return local(groups, n, gate, up, router_weight, router_gain)
        return plain(gate, up, router_weight, router_gain)

    in_specs = (
        P("expert", "shard", None),
        P("expert", "shard", None),
        P("shard", "expert"),
        P("shard"),
    )
    out_specs = (
        P("expert", None, "shard"),
        P("expert", None, "shard"),
        P("expert", "shard"),
        P("expert", "shard"),
        P(),
    )
    step = jax.shard_map(body, mesh=mesh, in_specs=in_specs, out_specs=out_specs, check_vma=False)

    def whole(master_gate, master_up, router_weight, router_gain):
        experts, rows, cols = master_gate.shape
        run = step
        if suits(groups, n, experts // groups, rows // n, cols):
            run = step
        return run(master_gate, master_up, router_weight, router_gain)

    return whole
```

```python
import jax
import jax.numpy as jnp
from jax import lax
from jax.experimental import pallas as pl
from jax.experimental.pallas import tpu as pltpu
from jax.sharding import PartitionSpec as P


GRANT = 48 * 1024 * 1024
SMALL = 8 * 1024 * 1024
SPAN = 248.0
HALF = 124.0
SPLIT = 4
TINY = 1.2e-19
LEAST, RATE, DEEP = 0.05, 240.0 / 8.2, 120.0
FAR = pl.BlockSpec(memory_space=pltpu.MemorySpace.HBM)


def plain(master_gate, master_up, router_weight, router_gain):
    total_gate, total_up = lax.psum(
        (jnp.sum(master_gate * master_gate, axis=1), jnp.sum(master_up * master_up, axis=1)),
        "shard",
    )
    scale_gate = jnp.sqrt(total_gate)
    scale_up = jnp.sqrt(total_up)
    narrow_gate = (master_gate / jnp.expand_dims(scale_gate, 1)).astype(jnp.bfloat16)
    narrow_up = (master_up / jnp.expand_dims(scale_up, 1)).astype(jnp.bfloat16)
    final_gate = lax.all_to_all(narrow_gate, "shard", split_axis=2, concat_axis=1, tiled=True)
    final_up = lax.all_to_all(narrow_up, "shard", split_axis=2, concat_axis=1, tiled=True)
    mine = lax.axis_index("shard") * final_gate.shape[2]
    scale_gate = lax.dynamic_slice_in_dim(scale_gate, mine, final_gate.shape[2], axis=1)
    scale_up = lax.dynamic_slice_in_dim(scale_up, mine, final_up.shape[2], axis=1)
    part_router = (router_weight * router_gain[:, None]).astype(jnp.bfloat16)
    row_router = lax.all_gather(part_router, "shard", axis=0, tiled=True)
    serve_router = lax.all_gather(row_router, "expert", axis=1, tiled=True)
    return (final_gate, final_up, scale_gate, scale_up, serve_router)


def column_max(x):
    return jnp.max(jnp.abs(x), axis=0, keepdims=True).astype(jnp.bfloat16).astype(jnp.float32)


def offsets(n):
    return (0, 6, 2, 4, 3, 5, 7, 1) if n == 8 else tuple(range(n))


def encode_kernel(n, piece, near, *refs):
    outs, turned = refs[-1 - n : -1], refs[-1]
    me = lax.axis_index("shard")
    x = jnp.concatenate([ref[0] for ref in refs[:SPLIT]], axis=0)
    top = column_max(x)
    step = jnp.where(top > TINY, SPAN / jnp.maximum(top, TINY), 0.0)
    y = jnp.exp2(jnp.abs(x) * step - HALF)
    y = jnp.where(x < 0, -y, y)
    turned[...] = y.astype(jnp.bfloat16).T
    at = pl.program_id(0) if near else 0
    for k, o in enumerate(offsets(n)):
        first = pl.multiple_of((me ^ o) * piece, 16)
        outs[k][at] = turned[pl.ds(first, piece), :]


def split_specs(rows, cols, first):
    return [
        pl.BlockSpec((1, rows // SPLIT, cols), lambda i, p=p: (first + i, p, 0))
        for p in range(SPLIT)
    ]


def encode(x, first, count, n, after=(), near=False):
    _, rows, cols = x.shape
    piece = cols // n
    block = jax.ShapeDtypeStruct((count, piece, rows), jnp.bfloat16)
    return pl.pallas_call(
        lambda *refs: encode_kernel(n, piece, near, *refs),
        name="encode",
        grid=(count,),
        out_shape=[block] * n,
        in_specs=split_specs(rows, cols, first) + [FAR] * len(after),
        out_specs=[
            pl.BlockSpec(memory_space=pltpu.MemorySpace.VMEM)
            if near
            else pl.BlockSpec((1, piece, rows), lambda i: (i, 0, 0))
        ]
        * n,
        scratch_shapes=[pltpu.VMEM((cols, rows), jnp.bfloat16)],
        compiler_params=pltpu.CompilerParams(vmem_limit_bytes=GRANT),
        cost_estimate=pl.CostEstimate(
            flops=count * 4_000_000, bytes_accessed=count * rows * cols * 6, transcendentals=0
        ),
    )(*[x] * SPLIT, *after)


def stats_kernel(n, piece, experts, *refs):
    gate_refs, up_refs = refs[:SPLIT], refs[SPLIT : 2 * SPLIT]
    router_ref, gain_ref = refs[2 * SPLIT : 2 * SPLIT + 2]
    outs = refs[-3 - n : -3]
    sums, tops, turned = refs[-3:]
    e = pl.program_id(0)
    me = lax.axis_index("shard")
    for k, parts in enumerate((gate_refs, up_refs)):
        x = jnp.concatenate([ref[0] for ref in parts], axis=0)
        sums[pl.ds(k * experts + e, 1), :] = jnp.sum(x * x, axis=0, keepdims=True)
        tops[pl.ds(k * experts + e, 1), :] = column_max(x)

    @pl.when(e == experts - 1)
    def _():
        top = tops[...]
        ratio = jnp.where(top > TINY, sums[...] / jnp.maximum(top * top, TINY * TINY), 1.0)
        code = jnp.exp2((jnp.log2(ratio) + LEAST) * RATE - DEEP)
        both = jnp.concatenate([code, top], axis=0)
        turned[...] = jnp.concatenate([both, both], axis=0).T
        router = (router_ref[...] * gain_ref[...]).astype(jnp.bfloat16)
        half = router.shape[1] // 2
        short = piece // 2
        lane = lax.broadcasted_iota(jnp.int32, (short, 128), 1)
        for k, o in enumerate(offsets(n)):
            first = pl.multiple_of((me ^ o) * piece, 8)
            one = turned[pl.ds(first, short), :]
            two = turned[pl.ds(pl.multiple_of(first + short, 8), short), :]
            outs[k][pl.ds(0, experts), :] = router[:, :half]
            outs[k][pl.ds(experts, experts), :] = router[:, half:]
            packed = jnp.where(lane < 64, one, two).astype(jnp.bfloat16)
            outs[k][pl.ds(2 * experts, short), :] = packed


def stats(gate, up, router, gain, n, after=()):
    experts, rows, cols = gate.shape
    piece = cols // n
    block = jax.ShapeDtypeStruct((piece // 2 + 2 * experts, 128), jnp.bfloat16)
    whole = pl.BlockSpec(memory_space=pltpu.VMEM)
    return pl.pallas_call(
        lambda *refs: stats_kernel(n, piece, experts, *refs),
        name="stats",
        grid=(experts,),
        out_shape=[block] * n,
        in_specs=split_specs(rows, cols, 0) * 2
        + [whole] * 2
        + [FAR] * len(after),
        out_specs=[whole] * n,
        scratch_shapes=[
            pltpu.VMEM((2 * experts, cols), jnp.float32),
            pltpu.VMEM((2 * experts, cols), jnp.float32),
            pltpu.VMEM((cols, 128), jnp.float32),
        ],
        compiler_params=pltpu.CompilerParams(vmem_limit_bytes=GRANT),
        cost_estimate=pl.CostEstimate(
            flops=experts * 4_000_000, bytes_accessed=experts * rows * cols * 8, transcendentals=0
        ),
    )(*[gate] * SPLIT, *[up] * SPLIT, router, gain, *after)


def factor_kernel(n, piece, experts, rows, *refs):
    told = refs[:n]
    factor_ref, gate_ref, up_ref, router_ref = refs[n:]
    me = lax.axis_index("shard")
    w = 2 * experts
    half, short = rows // 2, piece // 2
    total, tops = None, []
    for k, o in enumerate(offsets(n)):
        lines = told[k][pl.ds(2 * experts, short), :].astype(jnp.float32).T
        lines = jnp.concatenate([lines[: 2 * w], lines[2 * w :]], axis=1)
        top = lines[w:]
        ratio = jnp.exp2((jnp.log2(lines[:w]) + DEEP) / RATE - LEAST)
        part = ratio * (top * top)
        total = part if total is None else total + part
        tops.append(top)
        for h in range(2):
            at = pl.multiple_of((me ^ o) * rows + h * half, half)
            router_ref[:, pl.ds(at, half)] = told[k][pl.ds(h * experts, experts), :]
    scale = jnp.sqrt(total)
    gate_ref[...] = scale[:experts]
    up_ref[...] = scale[experts:]
    for k in range(n):
        factor_ref[:, k, :] = tops[k] / (SPAN * scale)


def factors(told, experts, rows, router_kind):
    n = len(told)
    piece = 2 * (told[0].shape[0] - 2 * experts)
    return pl.pallas_call(
        lambda *refs: factor_kernel(n, piece, experts, rows, *refs),
        name="factors",
        out_shape=[
            jax.ShapeDtypeStruct((2 * experts, n, piece), jnp.float32),
            jax.ShapeDtypeStruct((experts, piece), jnp.float32),
            jax.ShapeDtypeStruct((experts, piece), jnp.float32),
            jax.ShapeDtypeStruct((experts, n * rows), router_kind),
        ],
        compiler_params=pltpu.CompilerParams(vmem_limit_bytes=GRANT),
        cost_estimate=pl.CostEstimate(
            flops=2_000_000, bytes_accessed=3_000_000, transcendentals=0
        ),
    )(*told)


def decode_kernel(n, rows, *refs):
    factor_ref, pieces, out_ref, token_ref = refs[0], refs[1 : 1 + n], refs[-2], refs[-1]
    token_ref[...] = jnp.zeros_like(token_ref)
    me = lax.axis_index("shard")
    factor = factor_ref[0].T
    for k, o in enumerate(offsets(n)):
        first = pl.multiple_of((me ^ o) * rows, 128)
        out_ref[0, :, pl.ds(first, rows)] = decoded(pieces[k][0], factor[:, k : k + 1])


def decoded(y, factor):
    y = y.astype(jnp.float32)
    v = (jnp.log2(jnp.abs(y)) + HALF) * factor
    return jnp.where(y < 0, -v, v).astype(jnp.bfloat16)


def decode(pieces, factor, which, first, experts, into):
    n = len(pieces)
    count, piece, rows = pieces[0].shape
    base = which * experts + first
    into = () if into is None else (into,)
    return pl.pallas_call(
        lambda *refs: decode_kernel(n, rows, *refs),
        name="decode",
        grid=(count,),
        out_shape=[
            jax.ShapeDtypeStruct((experts, piece, n * rows), jnp.bfloat16),
            jax.ShapeDtypeStruct((8, 128), jnp.float32),
        ],
        in_specs=[pl.BlockSpec((1, n, piece), lambda i: (base + i, 0, 0))]
        + [pl.BlockSpec((1, piece, rows), lambda i: (i, 0, 0))] * n
        + [FAR] * len(into),
        out_specs=[
            pl.BlockSpec((1, piece, n * rows), lambda i: (first + i, 0, 0)),
            pl.BlockSpec((8, 128), lambda i: (0, 0)),
        ],
        input_output_aliases={n + 1: 0} if into else {},
        compiler_params=pltpu.CompilerParams(vmem_limit_bytes=GRANT),
        cost_estimate=pl.CostEstimate(
            flops=count * 4_000_000, bytes_accessed=count * rows * piece * n * 4, transcendentals=0
        ),
    )(factor, *pieces, *into)


def finish_kernel(n, some, base, which, rows, *refs):
    factor_ref, pieces = refs[0], refs[1 : 1 + len(some)]
    out_ref, token_ref, ready, sems = refs[-4:]
    token_ref[...] = jnp.zeros_like(token_ref)
    me = lax.axis_index("shard")
    factor = factor_ref[base].T
    copies = []
    for at, k in enumerate(some):
        first = pl.multiple_of((me ^ offsets(n)[k]) * rows, 128)
        ready[at] = decoded(pieces[at][0], factor[:, k : k + 1])
        copies.append(
            pltpu.make_async_copy(
                ready.at[at], out_ref.at[which, :, pl.ds(first, rows)], sems.at[at]
            )
        )
    for copy in copies:
        copy.start()
    for copy in copies:
        copy.wait()


def finish(pieces, some, factor, base, which, into):
    n = factor.shape[1]
    _, piece, rows = pieces[0].shape
    near = pl.BlockSpec(memory_space=pltpu.MemorySpace.VMEM)
    return pl.pallas_call(
        lambda *refs: finish_kernel(n, some, base, which, rows, *refs),
        name="finish",
        out_shape=[
            jax.ShapeDtypeStruct(into.shape, into.dtype),
            jax.ShapeDtypeStruct((8, 128), jnp.float32),
        ],
        in_specs=[near] * (1 + len(some)) + [FAR],
        out_specs=[FAR, near],
        scratch_shapes=[
            pltpu.VMEM((len(some), piece, rows), jnp.bfloat16),
            pltpu.SemaphoreType.DMA((len(some),)),
        ],
        input_output_aliases={len(some) + 1: 0},
        compiler_params=pltpu.CompilerParams(vmem_limit_bytes=SMALL),
        cost_estimate=pl.CostEstimate(
            flops=500_000 * len(some),
            bytes_accessed=rows * piece * len(some) * 4,
            transcendentals=0,
        ),
    )(factor, *pieces, into)


def place_kernel(axis, along, n, part, *refs):
    me = lax.axis_index(axis)
    out_ref = refs[-1]
    for o in range(n):
        first = pl.multiple_of((me ^ o) * part, part)
        at = (slice(None), pl.ds(first, part)) if along else (pl.ds(first, part), slice(None))
        out_ref[at] = refs[o][...]


def place(parts, axis, along):
    n = len(parts)
    shape = list(parts[0].shape)
    part = shape[along]
    shape[along] *= n
    return pl.pallas_call(
        lambda *refs: place_kernel(axis, along, n, part, *refs),
        name="place",
        out_shape=jax.ShapeDtypeStruct(tuple(shape), parts[0].dtype),
    )(*parts)


def swap(x, axis, n, o):
    return lax.ppermute(x, axis, [(i, i ^ o) for i in range(n)])


def exchange(parts):
    n = len(parts)
    return [parts[0]] + [
        swap(parts[k], "shard", n, o) for k, o in enumerate(offsets(n)) if o
    ]


def cuts(experts):
    sizes, left = [], experts
    step = max(1, experts // 4)
    while left > 0:
        sizes.append(min(step, left))
        left -= sizes[-1]
    return sizes


def plan(experts):
    if experts == 16:
        sizes = ([2, 5, 5, 4], [5, 5, 3, 2, 1])
    else:
        sizes = (cuts(experts), cuts(experts))
    chunks = []
    for which in range(2):
        first = 0
        for size in sizes[which]:
            chunks.append((which, first, size))
            first += size
    return chunks


AHEAD = 2
NEAR = (0, -1)


def local(groups, n, gate, up, router_weight, router_gain):
    experts, rows, _ = gate.shape
    chunks = plan(experts)
    source = (gate, up)
    result = [None, None]
    got, tokens = {}, {}

    def send(k):
        which, first, size = chunks[k]
        after = ()
        if k >= AHEAD:
            after += tuple(got[k - AHEAD][1:])
        if k - AHEAD - 1 in tokens:
            after += (tokens[k - AHEAD - 1],)
        if k == AHEAD + 3:
            after += (placed,)
        near = k in NEAR or k - len(chunks) in NEAR
        sent = encode(source[which], first, size, n, after, near)
        got[k] = exchange(sent)

    def receive(k):
        which, first, size = chunks[k]
        if size == 1 and k == len(chunks) - 1:
            base = which * experts + first
            late = tuple(range(n // 2, n - 1))
            soon = tuple(range(n // 2)) + (n - 1,)
            for some in (soon, late):
                pieces = [got[k][j] for j in some]
                result[which], tokens[k] = finish(pieces, some, factor, base, first, result[which])
            return
        result[which], tokens[k] = decode(
            got[k], factor, which, first, experts, result[which]
        )

    for k in range(AHEAD):
        send(k)
    messages = stats(gate, up, router_weight.T, router_gain[None, :], n)
    messages = exchange(messages)
    factor, scale_gate, scale_up, rows_router = factors(messages, experts, rows, jnp.bfloat16)
    blocks = [rows_router] + [
        swap(rows_router, "expert", groups, o) for o in range(1, groups)
    ]
    placed = place(blocks, "expert", 0)
    for k in range(AHEAD, len(chunks)):
        send(k)
        receive(k - AHEAD)
    for k in range(len(chunks) - AHEAD, len(chunks)):
        receive(k)
    return (
        result[0].transpose(0, 2, 1),
        result[1].transpose(0, 2, 1),
        scale_gate,
        scale_up,
        placed.T,
    )


def power_of_two(n):
    return n & (n - 1) == 0


def suits(groups, n, experts, rows, cols):
    return (
        power_of_two(n)
        and power_of_two(groups)
        and n <= 16
        and cols % (16 * n) == 0
        and cols % 128 == 0
        and rows == 256
        and experts == 16
    )


def solution(mesh):
    groups, n = mesh.shape["expert"], mesh.shape["shard"]

    def body(gate, up, router_weight, router_gain):
        if gate.shape == up.shape and suits(groups, n, *gate.shape):
            return local(groups, n, gate, up, router_weight, router_gain)
        return plain(gate, up, router_weight, router_gain)

    in_specs = (
        P("expert", "shard", None),
        P("expert", "shard", None),
        P("shard", "expert"),
        P("shard"),
    )
    out_specs = (
        P("expert", None, "shard"),
        P("expert", None, "shard"),
        P("expert", "shard"),
        P("expert", "shard"),
        P(),
    )
    step = jax.shard_map(body, mesh=mesh, in_specs=in_specs, out_specs=out_specs, check_vma=False)

    def whole(master_gate, master_up, router_weight, router_gain):
        experts, rows, cols = master_gate.shape
        run = step
        if suits(groups, n, experts // groups, rows // n, cols):
            run = step
        return run(master_gate, master_up, router_weight, router_gain)

    return whole
```
